256 devices in a mesh: groups: 4 (over x, y), ctx: 64 (over z, core).
Axes of the slice: x: 2, y: 2, z: 32, core: 2. Of those that a mesh axis runs over, the one named last changes fastest.
The devices are a block of a 4x8x32 slice.
Arguments:
- queries: bfloat16 [32768, 1024], P(('groups', 'ctx')), parts along dimension 0, may hold values from -27 to 27
- keys: bfloat16 [32768, 1024], P(('groups', 'ctx')), parts along dimension 0, may hold values from -6 to 6
- values: bfloat16 [32768, 1024], P(('groups', 'ctx')), parts along dimension 0, may hold values from -6 to 6
- resid: bfloat16 [32768, 2048], P(('groups', 'ctx')), parts along dimension 0, may hold values from -6 to 6
- out_proj: bfloat16 [1024, 2048], replicated, may hold values from -0.1875 to 0.1875
- norm_gain: float32 [2048], replicated, may hold values from 0.25 to 1.75
- up_proj: bfloat16 [2048, 4096], P(None, 'ctx'), may hold values from -0.125 to 0.125
- down_proj: bfloat16 [2048, 4096], P(None, 'ctx'), may hold values from -0.09375 to 0.09375
- router: bfloat16 [2048, 8], replicated, may hold values from -0.125 to 0.125
- expert_ids: int32 [32768, 1], P(('groups', 'ctx')), parts along dimension 0, may hold values from 0 to 7; in each aligned block of 128 rows (0 to 127, 128 to 255, ...) at most 20 rows name the same one
- expert_in: bfloat16 [64, 2048, 512], P('ctx'), may hold values from -0.125 to 0.125
- expert_out: bfloat16 [64, 512, 2048], P('ctx'), may hold values from -0.09375 to 0.09375
Outputs:
- layer_out: bfloat16 [32768, 2048], P(('groups', 'ctx')), parts along dimension 0
The draws below stay inside these ranges and needn't reach their ends.
There are 4 independent parts, one for each index of `groups`. The reference program is written for one: setup_inputs(seed, part) draws one part's arguments, and reference() takes and returns one part's arrays. A program takes and returns all parts, laid end to end along the dimension named above; an argument that names none is the same for every part. Nothing has to cross between parts.
Inputs may be any that keep to these rules, and one draw needn't show every extreme that they name: `expert_ids`: among the 128 tokens of one index of ctx, at most 20 name the same expert; in every draw some index of ctx has 20 tokens naming one expert.
All inputs are finite; a program needn't handle non-finite values.
Results may differ from the reference program's by a relative error of at most 0.0075.
Values may be sent and summed in bfloat16 or wider, within the bound.
A program may use at most 192 MiB of HBM per device.

```python
import math
import jax
import jax.numpy as jnp
import numpy as np
from jax import lax

D = 2048
HEADS = 8
DH = 128
MLP_HID = 4096
EXP_HID = 4096
SPLIT = 8
TOK_DEV = 128
LIVE = 8
CAP = 20
SEQ = 8192
N_CTX = 64


def attention_draws(key):
    query_key = jax.random.fold_in(key, 11)
    keys_key = jax.random.fold_in(key, 12)
    width = HEADS * DH
    query_draw = jnp.clip(3.0 * jax.random.normal(query_key, (SEQ, width), jnp.float32), -18.0, 18.0)
    keys_draw = jnp.clip(jax.random.normal(keys_key, (SEQ, width), jnp.float32), -6.0, 6.0)
    return (query_draw, keys_draw)


def draw_queries(key, part):
    return attention_draws(key)[0].astype(jnp.bfloat16)


def draw_keys(key, part):
    return attention_draws(key)[1].astype(jnp.bfloat16)


def block_scale(own_key, shape, pieces, low, largest):
    def one(axis_at, blocks):
        draws = jax.random.uniform(jax.random.fold_in(jax.random.fold_in(own_key, 6), axis_at), (blocks,), jnp.float32, low / len(pieces), largest / len(pieces))
        return jnp.repeat(jnp.exp(draws), shape[axis_at] // blocks).reshape((-1,) + (1,) * (len(shape) - axis_at - 1))

    factor_of = one(*pieces[0])
    for cut in pieces[1:]:
        factor_of = factor_of * one(*cut)
    return factor_of


def routed_block(own_key, own, number, rows, number_of, top, reach, skew):
    order = jax.random.permutation(own_key, number_of)
    packed, ordinary = shares(number_of, rows * top, reach, skew, True), shares(number_of, rows * top, reach, skew, False)
    places = jnp.arange(number_of)

    def named(lengths, offset_by):
        used = int((lengths > 0).sum())
        fixed = max(1, used // 4)
        shifted = fixed + (places - fixed + offset_by * (used - fixed)) % max(1, number_of - fixed)
        return jnp.zeros((number_of,), jnp.int32).at[order[jnp.where(places < fixed, places, shifted)]].set(jnp.asarray(lengths, jnp.int32))

    lengths = jnp.where(number % 4 == 0, named(packed, number // 4), named(ordinary, number - number // 4 - 1))
    mixed = jax.random.permutation(jax.random.fold_in(own, 3), number_of)
    source_of, sink = mixed[0:number_of // 2 * 2:2], mixed[1:number_of // 2 * 2:2]
    slack = jnp.minimum(lengths[source_of] - 1, reach - lengths[sink]) // 2
    slack = jnp.where((source_of == order[0]) | (sink == order[0]) | (lengths[sink] == 0), 0, jnp.maximum(slack, 0))
    shifted = jax.random.randint(jax.random.fold_in(own, 4), (number_of // 2,), 0, 1 << 20) % (slack + 1)
    lengths = lengths.at[source_of].add(-shifted).at[sink].add(shifted)
    labels = jnp.searchsorted(jnp.cumsum(lengths), jnp.arange(rows * top), side="right").astype(jnp.int32)
    grid = labels.reshape(top, rows).T
    grid = grid[jax.random.permutation(jax.random.fold_in(own, 1), rows)]
    offset_by = jax.random.randint(jax.random.fold_in(own, 2), (rows, 1), 0, top)
    return jnp.take_along_axis(grid, (jnp.arange(top)[None, :] + offset_by) % top, axis=1)


def shares(number_of, total, reach, slope, full):
    loads = [(1 << 20) // math.isqrt(standing ** slope) + 1 for standing in range(1, number_of + 1)]
    largest = reach if full else min(reach, max(-(-total // number_of), total * loads[0] // sum(loads)))
    least = 1 if total - largest >= number_of - 1 else 0
    counts, spare = [largest] + [least] * (number_of - 1), total - largest - least * (number_of - 1)
    while spare > 0:
        movable = [i for i in range(1, number_of) if counts[i] < largest] or [i for i in range(1, number_of) if counts[i] < reach]
        mass, remaining = sum([loads[i] for i in movable]), spare
        for i in movable:
            addition = min(reach - counts[i], max(1, remaining * loads[i] // mass), spare)
            counts[i] = counts[i] + addition
            spare = spare - addition
    return np.array(counts)


def noise(own_key, extent, deviation, most, shards=(), kind=jnp.bfloat16):
    loudness = block_scale(own_key, extent, shards, -0.22, 0.18) if shards else 1.0
    entries = jax.random.normal(own_key, extent, jnp.float32) * deviation * loudness
    return jnp.minimum(jnp.maximum(entries, -most), most).astype(kind)


def setup_inputs(seed: int = 0, part: int = 0) -> dict:
    splits = jax.random.split(jax.random.key(seed), 13)
    part_keys = jax.random.split(jax.random.fold_in(splits[12], part), 13)
    queries = draw_queries(jax.random.fold_in(jax.random.fold_in(splits[12], part), 71), part)
    keys = draw_keys(jax.random.fold_in(jax.random.fold_in(splits[12], part), 71), part)
    values = noise(part_keys[2], (SEQ, HEADS * DH), 1.0, 6.0, ((0, 64),))
    resid = noise(part_keys[3], (SEQ, D), 1.0, 6.0, ((0, 64),))
    out_proj = noise(splits[4], (HEADS * DH, D), (HEADS * DH) ** -0.5, 0.1875)
    norm_gain = jnp.clip(1.0 + 0.15 * jax.random.normal(splits[5], (D,), jnp.float32), 0.25, 1.75)
    up_proj = noise(splits[6], (D, MLP_HID), D ** -0.5, 0.125, ((1, 64),))
    down_proj = noise(splits[7], (D, MLP_HID), MLP_HID ** -0.5, 0.09375, ((1, 64),))
    router = noise(splits[8], (D, LIVE), D ** -0.5, 0.125)
    expert_ids_keys = jax.random.split(jax.random.fold_in(part_keys[9], 1), SEQ // TOK_DEV)
    expert_ids_turns = jax.random.permutation(jax.random.fold_in(part_keys[9], 3), SEQ // TOK_DEV)
    expert_ids = jax.vmap(lambda own, number: routed_block(jax.random.fold_in(part_keys[9], 2), own, number, TOK_DEV, LIVE, 1, CAP, 2))(expert_ids_keys, expert_ids_turns).reshape((SEQ, 1))
    expert_in = noise(splits[10], (SPLIT * LIVE, D, EXP_HID // SPLIT), D ** -0.5, 0.125, ((0, 64),))
    expert_out = noise(splits[11], (SPLIT * LIVE, EXP_HID // SPLIT, D), EXP_HID ** -0.5, 0.09375, ((0, 64),))
    return dict(queries=queries, keys=keys, values=values, resid=resid, out_proj=out_proj, norm_gain=norm_gain, up_proj=up_proj, down_proj=down_proj, router=router, expert_ids=expert_ids, expert_in=expert_in, expert_out=expert_out)


NEG_FILL = -1e+30
EPSILON = 1e-06

def reference(queries, keys, values, resid, out_proj, norm_gain, up_proj, down_proj, router, expert_ids, expert_in, expert_out):
    total_rows = queries.shape[0]
    key_heads = keys.astype(jnp.float32).reshape(total_rows, HEADS, DH)
    value_heads = values.astype(jnp.float32).reshape(total_rows, HEADS, DH)
    query_blocks = queries.reshape(N_CTX, TOK_DEV, HEADS, DH)
    key_positions = jnp.arange(total_rows, dtype=jnp.int32)

    def attend_block(operands):
        block_rows, block_index = operands
        scores = jnp.einsum('qhd,khd->hqk', block_rows.astype(jnp.float32), key_heads) * DH ** (-0.5)
        query_positions = block_index * TOK_DEV + jnp.arange(TOK_DEV, dtype=jnp.int32)
        visible = (key_positions[None, :] <= query_positions[:, None])[None]
        masked = jnp.where(visible, scores, NEG_FILL)
        row_max = lax.optimization_barrier(jnp.max(masked, axis=2))
        weights = jnp.where(visible, jnp.exp(masked - row_max[..., None]), 0.0)
        totals = lax.optimization_barrier(jnp.sum(weights, axis=2))
        numer = jnp.einsum('hqk,khd->hqd', weights.astype(jnp.bfloat16).astype(jnp.float32), value_heads)
        result = (numer / totals[..., None]).astype(jnp.bfloat16)
        return jnp.transpose(result, (1, 0, 2)).reshape(TOK_DEV, HEADS * DH)
    attn = lax.map(attend_block, (query_blocks, jnp.arange(N_CTX, dtype=jnp.int32))).reshape(total_rows, HEADS * DH)
    mixed = resid.astype(jnp.float32) + jnp.dot(attn, out_proj, preferred_element_type=jnp.float32)
    normed = (mixed * lax.rsqrt(lax.optimization_barrier(jnp.mean(mixed * mixed, axis=1, keepdims=True)) + EPSILON) * norm_gain).astype(jnp.bfloat16)
    chosen = expert_ids[:, 0]
    onehot = (chosen[:, None] == jnp.arange(LIVE, dtype=jnp.int32)[None, :]).astype(jnp.float32)
    logits = jnp.dot(normed, router, preferred_element_type=jnp.float32)
    gate = jax.nn.sigmoid(lax.optimization_barrier(jnp.sum(onehot * logits, axis=1)))
    block_units = EXP_HID // SPLIT
    mlp_units = MLP_HID // SPLIT
    full_in = jnp.transpose(expert_in.reshape(SPLIT, LIVE, D, block_units), (1, 2, 0, 3)).reshape(LIVE, D, EXP_HID)
    full_out = jnp.transpose(expert_out.reshape(SPLIT, LIVE, block_units, D), (1, 0, 2, 3)).reshape(LIVE, EXP_HID, D)
    grouped = onehot.reshape(N_CTX, TOK_DEV, LIVE)
    earlier = jnp.cumsum(grouped, axis=1) - grouped
    slot_index = lax.optimization_barrier(jnp.sum(earlier * grouped, axis=2)).reshape(total_rows).astype(jnp.int32)
    owner_index = (jnp.arange(total_rows, dtype=jnp.int32) // TOK_DEV).astype(jnp.int32)
    buffer_index = chosen * (N_CTX * CAP) + owner_index * CAP + slot_index
    buffer_rows = jnp.zeros((LIVE * N_CTX * CAP, D), jnp.bfloat16).at[buffer_index].set(normed)
    buffer_rows = buffer_rows.reshape(LIVE, N_CTX * CAP, D)
    gate_rows = jnp.zeros((LIVE * N_CTX * CAP,), jnp.float32).at[buffer_index].set(gate).reshape(LIVE, N_CTX * CAP)

    def apply_expert(operands):
        rows_in, gate_in, weight_in, weight_out = operands
        total = jnp.zeros((rows_in.shape[0], D), jnp.float32)
        for block in range(SPLIT):
            expert_low = block * block_units
            mlp_low = block * mlp_units
            expert_hidden = jax.nn.gelu(jnp.dot(rows_in, weight_in[:, expert_low:expert_low + block_units], preferred_element_type=jnp.float32)).astype(jnp.bfloat16)
            mlp_hidden = jax.nn.gelu(jnp.dot(rows_in, up_proj[:, mlp_low:mlp_low + mlp_units], preferred_element_type=jnp.float32)).astype(jnp.bfloat16)
            block_part = gate_in[:, None] * jnp.dot(expert_hidden, weight_out[expert_low:expert_low + block_units], preferred_element_type=jnp.float32)
            block_part = block_part + lax.dot_general(mlp_hidden, down_proj[:, mlp_low:mlp_low + mlp_units], (((1,), (1,)), ((), ())), preferred_element_type=jnp.float32)
            rounded = lax.optimization_barrier(block_part.astype(jnp.bfloat16))
            total = total + rounded.astype(jnp.float32)
        return total
    expert_rows = lax.map(apply_expert, (buffer_rows, gate_rows, full_in, full_out)).reshape(LIVE * N_CTX * CAP, D)
    mixture_part = expert_rows[buffer_index]
    return (mixed + mixture_part).astype(jnp.bfloat16)
```

```python
import functools
import jax
import jax.numpy as jnp
from jax import lax
from jax.experimental import pallas as pl
from jax.experimental.pallas import tpu as pltpu
from jax.sharding import PartitionSpec as P

DH = 128
SPLIT = 8
NEG_FILL = -1e30
EPSILON = 1e-06
LOG2E = 1.4426950408889634
KEY_BLOCK = 1024
QUERY_BLOCK = 256


def attend_kernel(members, tok_rows, q_ref, k_ref, v_ref, o_ref):
    pair = pl.program_id(0)
    member = lax.rem(lax.axis_index("ctx"), members)
    q = q_ref[...]
    segment = members * tok_rows
    scale = DH ** (-0.5) * LOG2E

    def block(begin, carry, masked):
        best, total, numer = carry
        keys = k_ref[pl.ds(begin, KEY_BLOCK), :]
        values = v_ref[pl.ds(begin, KEY_BLOCK), :]
        s = lax.dot_general(q, keys, (((1,), (1,)), ((), ())), preferred_element_type=jnp.float32)
        s = s * scale
        if masked:
            row = lax.broadcasted_iota(jnp.int32, s.shape, 0) + pair * QUERY_BLOCK
            at = (row // tok_rows) * segment + member * tok_rows + row % tok_rows
            key_at = lax.broadcasted_iota(jnp.int32, s.shape, 1) + begin
            s = jnp.where(key_at <= at, s, NEG_FILL)
        new_best = jnp.maximum(best, jnp.max(s, axis=1, keepdims=True))
        p = jnp.exp2(s - new_best)
        factor = jnp.exp2(best - new_best)
        total = total * factor + jnp.sum(p, axis=1, keepdims=True)
        numer = numer * factor + jnp.dot(
            p.astype(jnp.bfloat16), values, preferred_element_type=jnp.float32
        )
        return new_best, total, numer

    carry = (
        jnp.full((QUERY_BLOCK, 1), NEG_FILL, jnp.float32),
        jnp.zeros((QUERY_BLOCK, 1), jnp.float32),
        jnp.zeros((QUERY_BLOCK, DH), jnp.float32),
    )
    per_block = QUERY_BLOCK // tok_rows * segment // KEY_BLOCK
    carry = lax.fori_loop(
        0,
        pair * per_block,
        lambda i, c: block(pl.multiple_of(i * KEY_BLOCK, KEY_BLOCK), c, False),
        carry,
    )
    for extra in range(per_block):
        carry = block(
            pl.multiple_of((pair * per_block + extra) * KEY_BLOCK, KEY_BLOCK), carry, True
        )
    _, total, numer = carry
    o_ref[...] = (numer / total).astype(o_ref.dtype)


def attend(q, k, v, members, tok_rows):
    rows = q.shape[0]
    whole = pl.BlockSpec(k.shape, lambda i: (0, 0))
    return pl.pallas_call(
        functools.partial(attend_kernel, members, tok_rows),
        out_shape=jax.ShapeDtypeStruct(q.shape, jnp.bfloat16),
        grid=(rows // QUERY_BLOCK,),
        in_specs=[pl.BlockSpec((QUERY_BLOCK, DH), lambda i: (i, 0)), whole, whole],
        out_specs=pl.BlockSpec((QUERY_BLOCK, DH), lambda i: (i, 0)),
        cost_estimate=pl.CostEstimate(flops=10**10, bytes_accessed=5 * 10**6, transcendentals=5 * 10**6),
    )(q, k, v)


def body(
    queries,
    keys,
    values,
    resid,
    out_proj,
    norm_gain,
    up_proj,
    down_proj,
    router,
    expert_ids,
    expert_in,
    expert_out,
):
    tok_rows = queries.shape[0]
    heads = queries.shape[1] // DH
    width = resid.shape[1]
    live_count = router.shape[1]
    ctx_count = lax.axis_size("ctx")
    members = ctx_count // heads
    device_index = lax.axis_index("ctx")
    across = [[h * members + m for h in range(heads)] for m in range(members)]
    within = [[h * members + m for m in range(members)] for h in range(heads)]

    mlp_piece = jnp.stack([up_proj.T, down_proj.T], 0)
    qkv = jnp.stack([queries, keys, values], 0).reshape(3, tok_rows, heads, DH)
    qkv = jnp.transpose(qkv, (2, 0, 1, 3))
    mine = lax.all_to_all(
        qkv, "ctx", split_axis=0, concat_axis=0, tiled=True, axis_index_groups=across
    )
    q = mine[:, 0].reshape(heads * tok_rows, DH)
    kv = lax.all_gather(mine[:, 1:], "ctx", axis=0, axis_index_groups=within)
    k = jnp.transpose(kv[:, :, 0], (1, 0, 2, 3)).reshape(-1, DH)
    v = jnp.transpose(kv[:, :, 1], (1, 0, 2, 3)).reshape(-1, DH)
    mlp = lax.all_gather(mlp_piece, "ctx", axis=0, axis_index_groups=within)
    up_t = mlp[:, 0].reshape(-1, width)
    down_t = mlp[:, 1].reshape(-1, width)

    o = attend(q, k, v, members, tok_rows).reshape(heads, tok_rows, DH)
    o = lax.all_to_all(
        o, "ctx", split_axis=0, concat_axis=0, tiled=True, axis_index_groups=across
    )
    attn = jnp.transpose(o, (1, 0, 2)).reshape(tok_rows, heads * DH)

    mixed = resid.astype(jnp.float32) + jnp.dot(attn, out_proj, preferred_element_type=jnp.float32)
    normed = (
        mixed * lax.rsqrt(jnp.mean(mixed * mixed, axis=1, keepdims=True) + EPSILON) * norm_gain
    ).astype(jnp.bfloat16)

    slots_per = max(2, 5 * tok_rows // (4 * live_count))
    chosen = expert_ids[:, 0]
    onehot = (chosen[:, None] == jnp.arange(live_count, dtype=jnp.int32)[None, :]).astype(
        jnp.bfloat16
    )
    row_iota = jnp.arange(tok_rows, dtype=jnp.int32)
    strictly_lower = (row_iota[None, :] < row_iota[:, None]).astype(jnp.bfloat16)
    counts_before = jnp.dot(strictly_lower, onehot, preferred_element_type=jnp.float32)
    slot_index = jnp.sum(onehot.astype(jnp.float32) * counts_before, axis=1).astype(jnp.int32)
    target_slot = chosen * slots_per + slot_index
    own_expert = device_index % live_count
    all_slots = lax.all_gather(target_slot, "ctx", axis=0)
    tokens = lax.all_gather(normed, "ctx", axis=0)
    select = (
        all_slots[:, None, :]
        == (own_expert * slots_per + jnp.arange(slots_per, dtype=jnp.int32))[None, :, None]
    ).astype(jnp.bfloat16)
    rows = (
        jnp.einsum("jst,jtw->jsw", select, tokens, preferred_element_type=jnp.float32)
        .astype(jnp.bfloat16)
        .reshape(-1, width)
    )
    router_column = lax.dynamic_slice_in_dim(router, own_expert, 1, 1)
    weight_in = expert_in[0]
    weight_out = expert_out[0]
    expert_hidden = jax.nn.gelu(
        jnp.dot(rows, weight_in, preferred_element_type=jnp.float32)
    ).astype(jnp.bfloat16)
    mlp_hidden = jax.nn.gelu(
        lax.dot_general(rows, up_t, (((1,), (1,)), ((), ())), preferred_element_type=jnp.float32)
    ).astype(jnp.bfloat16)
    gate = jax.nn.sigmoid(jnp.dot(rows, router_column, preferred_element_type=jnp.float32))
    produced = gate * jnp.dot(expert_hidden, weight_out, preferred_element_type=jnp.float32)
    produced = produced + jnp.dot(mlp_hidden, down_t, preferred_element_type=jnp.float32)
    produced = produced.astype(jnp.bfloat16).reshape(ctx_count, slots_per, width)
    spread = jnp.einsum("jst,jsw->jtw", select, produced, preferred_element_type=jnp.float32)
    spread = spread.astype(jnp.bfloat16).reshape(ctx_count * tok_rows, width)
    summed = lax.psum_scatter(spread, "ctx", scatter_dimension=0, tiled=True)
    return (mixed + summed.astype(jnp.float32)).astype(jnp.bfloat16)


def solution(mesh):
    placed = (
        P(("groups", "ctx"), None),
        P(("groups", "ctx"), None),
        P(("groups", "ctx"), None),
        P(("groups", "ctx"), None),
        P(),
        P(),
        P(None, "ctx"),
        P(None, "ctx"),
        P(),
        P(("groups", "ctx"), None),
        P("ctx", None, None),
        P("ctx", None, None),
    )
    return jax.shard_map(
        body, mesh=mesh, in_specs=placed, out_specs=P(("groups", "ctx"), None), check_vma=False
    )
```

```python
import functools
import jax
import jax.numpy as jnp
from jax import lax
from jax.experimental import pallas as pl
from jax.experimental.pallas import tpu as pltpu
from jax.sharding import PartitionSpec as P

DH = 128
SPLIT = 8
NEG_FILL = -1e30
EPSILON = 1e-06
LOG2E = 1.4426950408889634
KEY_BLOCK = 1024
QUERY_BLOCK = 256
HALVES = 2
SOURCES = 8


def attend_kernel(members, tok_rows, q_ref, k_ref, v_ref, o_ref):
    pair = pl.program_id(0)
    member = lax.rem(lax.axis_index("ctx"), members)
    q = q_ref[...]
    segment = members * tok_rows
    scale = DH ** (-0.5) * LOG2E

    def block(begin, carry, masked):
        best, total, numer = carry
        keys = k_ref[pl.ds(begin, KEY_BLOCK), :]
        values = v_ref[pl.ds(begin, KEY_BLOCK), :]
        s = lax.dot_general(q, keys, (((1,), (1,)), ((), ())), preferred_element_type=jnp.float32)
        s = s * scale
        if masked:
            row = lax.broadcasted_iota(jnp.int32, s.shape, 0) + pair * QUERY_BLOCK
            at = (row // tok_rows) * segment + member * tok_rows + row % tok_rows
            key_at = lax.broadcasted_iota(jnp.int32, s.shape, 1) + begin
            s = jnp.where(key_at <= at, s, NEG_FILL)
        new_best = jnp.maximum(best, jnp.max(s, axis=1, keepdims=True))
        p = jnp.exp2(s - new_best)
        factor = jnp.exp2(best - new_best)
        total = total * factor + jnp.sum(p, axis=1, keepdims=True)
        numer = numer * factor + jnp.dot(
            p.astype(jnp.bfloat16), values, preferred_element_type=jnp.float32
        )
        return new_best, total, numer

    carry = (
        jnp.full((QUERY_BLOCK, 1), NEG_FILL, jnp.float32),
        jnp.zeros((QUERY_BLOCK, 1), jnp.float32),
        jnp.zeros((QUERY_BLOCK, DH), jnp.float32),
    )
    per_block = QUERY_BLOCK // tok_rows * segment // KEY_BLOCK
    carry = lax.fori_loop(
        0,
        pair * per_block,
        lambda i, c: block(pl.multiple_of(i * KEY_BLOCK, KEY_BLOCK), c, False),
        carry,
    )
    for extra in range(per_block):
        carry = block(
            pl.multiple_of((pair * per_block + extra) * KEY_BLOCK, KEY_BLOCK), carry, True
        )
    _, total, numer = carry
    o_ref[...] = (numer / total).astype(o_ref.dtype)


def attend(q, k, v, members, tok_rows):
    rows = q.shape[0]
    whole = pl.BlockSpec(k.shape, lambda i: (0, 0))
    return pl.pallas_call(
        functools.partial(attend_kernel, members, tok_rows),
        out_shape=jax.ShapeDtypeStruct(q.shape, jnp.bfloat16),
        grid=(rows // QUERY_BLOCK,),
        in_specs=[pl.BlockSpec((QUERY_BLOCK, DH), lambda i: (i, 0)), whole, whole],
        out_specs=pl.BlockSpec((QUERY_BLOCK, DH), lambda i: (i, 0)),
        cost_estimate=pl.CostEstimate(flops=10**10, bytes_accessed=5 * 10**6, transcendentals=5 * 10**6),
    )(q, k, v)


def gelu(x):
    return x * (0.5 * (1.0 + jnp.tanh(0.7978845608028654 * (x + 0.044715 * (x * x * x)))))


def mixture_kernel(
    token_ref, row_ref, column_ref, router_ref, in_ref, out_ref, up_ref, down_ref, spread_ref, slots
):
    block = token_ref.shape[0]
    pick = lax.broadcasted_iota(jnp.int32, (slots, block), 0) == row_ref[0]
    pick = jnp.where(pick, 1.0, 0.0).astype(jnp.bfloat16)
    rows = jnp.dot(pick, token_ref[...], preferred_element_type=jnp.float32)
    gate = jax.nn.sigmoid(jnp.sum(rows * router_ref[...], axis=1, keepdims=True))
    rows = rows.astype(jnp.bfloat16)
    expert_hidden = gelu(
        jnp.dot(rows, in_ref[...], preferred_element_type=jnp.float32)
    ).astype(jnp.bfloat16)
    mlp_hidden = gelu(
        lax.dot_general(
            rows, up_ref[...], (((1,), (1,)), ((), ())), preferred_element_type=jnp.float32
        )
    ).astype(jnp.bfloat16)
    produced = gate * jnp.dot(expert_hidden, out_ref[...], preferred_element_type=jnp.float32)
    produced = produced + jnp.dot(mlp_hidden, down_ref[...], preferred_element_type=jnp.float32)
    put = lax.broadcasted_iota(jnp.int32, (block, slots), 1) == column_ref[...]
    put = jnp.where(put, 1.0, 0.0).astype(jnp.bfloat16)
    spread_ref[...] = jnp.dot(
        put, produced.astype(jnp.bfloat16), preferred_element_type=jnp.float32
    ).astype(spread_ref.dtype)


def mixture(tokens, local_row, router_row, weight_in, weight_out, up_t, down_t, slots_per):
    count, width = tokens.shape
    half_rows = local_row.shape[1]
    block = SOURCES * half_rows
    slots = SOURCES * slots_per
    steps = count // block

    def kernel(*refs):
        mixture_kernel(*refs, slots)

    def fixed(a):
        return pl.BlockSpec(a.shape, lambda i: (0, 0))

    return pl.pallas_call(
        kernel,
        out_shape=jax.ShapeDtypeStruct((count, width), jnp.bfloat16),
        grid=(steps,),
        in_specs=[
            pl.BlockSpec((block, width), lambda i: (i, 0)),
            pl.BlockSpec((1, 1, block), lambda i: (i, 0, 0)),
            pl.BlockSpec((block, 1), lambda i: (i, 0)),
            fixed(router_row),
            fixed(weight_in),
            fixed(weight_out),
            fixed(up_t),
            fixed(down_t),
        ],
        out_specs=pl.BlockSpec((block, width), lambda i: (i, 0)),
        cost_estimate=pl.CostEstimate(
            flops=2 * steps * slots * width * (4 * weight_in.shape[1] + 2 * block),
            bytes_accessed=4 * count * width + 8 * weight_in.size,
            transcendentals=2 * steps * slots * weight_in.shape[1],
        ),
    )(
        tokens,
        local_row.reshape(steps, 1, block),
        local_row.reshape(count, 1),
        router_row,
        weight_in,
        weight_out,
        up_t,
        down_t,
    )


def body(
    queries,
    keys,
    values,
    resid,
    out_proj,
    norm_gain,
    up_proj,
    down_proj,
    router,
    expert_ids,
    expert_in,
    expert_out,
):
    tok_rows = queries.shape[0]
    heads = queries.shape[1] // DH
    width = resid.shape[1]
    live_count = router.shape[1]
    ctx_count = lax.axis_size("ctx")
    members = ctx_count // heads
    device_index = lax.axis_index("ctx")
    across = [[h * members + m for h in range(heads)] for m in range(members)]
    within = [[h * members + m for m in range(members)] for h in range(heads)]

    mlp_piece = jnp.stack([up_proj.T, down_proj.T], 0)
    qkv = jnp.stack([queries, keys, values], 0).reshape(3, tok_rows, heads, DH)
    qkv = jnp.transpose(qkv, (2, 0, 1, 3))
    mine = lax.all_to_all(
        qkv, "ctx", split_axis=0, concat_axis=0, tiled=True, axis_index_groups=across
    )
    q = mine[:, 0].reshape(heads * tok_rows, DH)
    kv = lax.all_gather(mine[:, 1:], "ctx", axis=0, axis_index_groups=within)
    k = jnp.transpose(kv[:, :, 0], (1, 0, 2, 3)).reshape(-1, DH)
    v = jnp.transpose(kv[:, :, 1], (1, 0, 2, 3)).reshape(-1, DH)
    mlp = lax.all_gather(mlp_piece, "ctx", axis=0, axis_index_groups=within)
    up_t = mlp[:, 0].reshape(-1, width)
    down_t = mlp[:, 1].reshape(-1, width)

    o = attend(q, k, v, members, tok_rows).reshape(heads, tok_rows, DH)
    o = lax.all_to_all(
        o, "ctx", split_axis=0, concat_axis=0, tiled=True, axis_index_groups=across
    )
    attn = jnp.transpose(o, (1, 0, 2)).reshape(tok_rows, heads * DH)

    mixed = resid.astype(jnp.float32) + jnp.dot(attn, out_proj, preferred_element_type=jnp.float32)
    normed = (
        mixed * lax.rsqrt(jnp.mean(mixed * mixed, axis=1, keepdims=True) + EPSILON) * norm_gain
    ).astype(jnp.bfloat16)

    slots_per = max(2, 5 * tok_rows // (4 * live_count))
    half_rows = tok_rows // HALVES
    chosen = expert_ids[:, 0]
    onehot = (chosen[:, None] == jnp.arange(live_count, dtype=jnp.int32)[None, :]).astype(
        jnp.bfloat16
    )
    row_iota = jnp.arange(tok_rows, dtype=jnp.int32)
    earlier = (row_iota[None, :] < row_iota[:, None]) & (
        row_iota[None, :] // half_rows == row_iota[:, None] // half_rows
    )
    counts_before = jnp.dot(
        earlier.astype(jnp.bfloat16), onehot, preferred_element_type=jnp.float32
    )
    slot_index = jnp.sum(onehot.astype(jnp.float32) * counts_before, axis=1).astype(jnp.int32)
    target_slot = chosen * slots_per + slot_index
    own_expert = device_index % live_count
    tokens = [
        lax.all_gather(normed[h * half_rows : (h + 1) * half_rows], "ctx", axis=0, tiled=True)
        for h in range(HALVES)
    ]
    all_slots = lax.all_gather(target_slot, "ctx", axis=0)
    local_slot = all_slots - own_expert * slots_per
    source = jnp.arange(ctx_count, dtype=jnp.int32)[:, None] % SOURCES
    local_row = jnp.where(
        (local_slot >= 0) & (local_slot < slots_per), source * slots_per + local_slot, -1
    )
    router_row = lax.dynamic_slice_in_dim(router, own_expert, 1, 1).T.astype(jnp.float32)
    summed = []
    for h in range(HALVES):
        rows_here = local_row[:, h * half_rows : (h + 1) * half_rows]
        spread = mixture(
            tokens[h],
            rows_here,
            router_row,
            expert_in[0],
            expert_out[0],
            up_t,
            down_t,
            slots_per,
        )
        summed.append(lax.psum_scatter(spread, "ctx", scatter_dimension=0, tiled=True))
    summed = jnp.concatenate(summed, axis=0)
    return (mixed + summed.astype(jnp.float32)).astype(jnp.bfloat16)


def solution(mesh):
    placed = (
        P(("groups", "ctx"), None),
        P(("groups", "ctx"), None),
        P(("groups", "ctx"), None),
        P(("groups", "ctx"), None),
        P(),
        P(),
        P(None, "ctx"),
        P(None, "ctx"),
        P(),
        P(("groups", "ctx"), None),
        P("ctx", None, None),
        P("ctx", None, None),
    )
    return jax.shard_map(
        body, mesh=mesh, in_specs=placed, out_specs=P(("groups", "ctx"), None), check_vma=False
    )
```
